32 devices in a mesh: groups: 2 (over y), queue: 8 (over z, x), tp: 2 (over core).
Axes of the slice: x: 2, y: 2, z: 4, core: 2. Of those that a mesh axis runs over, the one named last changes fastest.
Arguments:
- hidden: bfloat16 [3328, 5120], P(('groups', 'queue'), 'tp'), parts along dimension 0, may hold values from -8 to 8
- q_weight: bfloat16 [1, 40, 128, 128], P(None, 'tp'), may hold values from -1 to 2.5
- k_weight: bfloat16 [1, 40, 128, 128], P(None, 'tp'), may hold values from -1 to 2.5
- v_weight: bfloat16 [1, 40, 128, 128], P(None, 'tp'), may hold values from -0.5 to 0.5
- mod_base: float32 [1, 3, 5120], P(None, None, 'tp'), may hold values from -3 to 3
- mod_amp: float32 [1, 3, 5120], P(None, None, 'tp'), may hold values from -3 to 3
- levels: int32 [16], P(('groups', 'queue')), parts along dimension 0, may hold values from 0 to 63
- steps_table: int32 [65], replicated, may hold values from 0 to 1000
- group_pos: int32 [16], P('groups'), parts along dimension 0, may hold values from 0 to 31
Outputs:
- new_queue: bfloat16 [3328, 5120], P(('groups', 'queue'), 'tp'), parts along dimension 0
- velocity: bfloat16 [3328, 5120], P(('groups', 'queue'), 'tp'), parts along dimension 0
The draws below stay inside these ranges and needn't reach their ends.
There are 2 independent parts, one for each index of `groups`. The reference program is written for one: setup_inputs(seed, part) draws one part's arguments, and reference() takes and returns one part's arrays. A program takes and returns all parts, laid end to end along the dimension named above; an argument that names none is the same for every part. Nothing has to cross between parts.
All inputs are finite; a program needn't handle non-finite values.
Results may differ from the reference program's by a relative error of at most 0.0054.
Values may be sent and summed in bfloat16 or wider, within the bound.
A program may use at most 64 MiB of HBM per device.

```python
import math
import jax
import jax.numpy as jnp
from jax import lax

HEADS = 40
HEAD = 128
D = 5120
WIDE = 52
HW_DEV = 104
TOK_DEV = 208
BLOCKS = 1
STEPS = 64
QUEUE = 8
TOKENS = 1664


def draw_hidden(key, part):
    keys = jax.random.split(jax.random.fold_in(key, 11), 1)
    result = jnp.clip(jax.random.normal(keys[0], (TOKENS, D), jnp.float32), -6.0, 6.0)
    return result.astype(jnp.bfloat16)


def head_map(key):
    noise = jnp.clip(jax.random.normal(key, (BLOCKS, HEADS, HEAD, HEAD), jnp.float32), -6.0, 6.0)
    diag = 0.3
    noise = noise / jnp.sqrt(jnp.float32(HEAD))
    ident = jnp.eye(HEAD, dtype=jnp.float32)
    return (noise + diag * ident[None, None]).astype(jnp.bfloat16)


def draw_q_weight(key, part):
    return head_map(jax.random.fold_in(key, 23))


def draw_k_weight(key, part):
    return head_map(jax.random.fold_in(key, 37))


def with_ends(values, key, low, largest):
    spot = [jax.random.randint(jax.random.fold_in(key, axis), (), 0, length) for axis, length in enumerate(values.shape)]
    widest = values.shape.index(max(values.shape))
    neighbour = spot[:widest] + [(spot[widest] + 1) % values.shape[widest]] + spot[widest + 1:]
    return values.at[tuple(spot)].set(low).at[tuple(neighbour)].set(largest)


def block_levels(own_key, extent, pieces, smallest, largest):
    def one(dim, blocks):
        steps = jax.random.uniform(jax.random.fold_in(jax.random.fold_in(own_key, 6), dim), (blocks,), jnp.float32, smallest / len(pieces), largest / len(pieces))
        return jnp.repeat(jnp.exp(steps), extent[dim] // blocks).reshape((-1,) + (1,) * (len(extent) - dim - 1))

    factor_of = one(*pieces[0])
    for cut in pieces[1:]:
        factor_of = factor_of * one(*cut)
    return factor_of


def gaussian(key, dims, deviation, reach, cuts=(), kind=jnp.bfloat16):
    drawn = deviation * jax.random.normal(key, dims, jnp.float32)
    if cuts:
        drawn = drawn * block_levels(key, dims, cuts, -0.22, 0.18)
    return jnp.clip(drawn, -reach, reach).astype(kind)


def setup_inputs(seed: int = 0, part: int = 0) -> dict:
    streams_of = jax.random.split(jax.random.key(seed), 10)
    part_keys = jax.random.split(jax.random.fold_in(streams_of[9], part), 10)
    return {
        "hidden": draw_hidden(jax.random.fold_in(jax.random.fold_in(streams_of[9], part), 71), part),
        "q_weight": draw_q_weight(jax.random.fold_in(streams_of[9], 71), part),
        "k_weight": draw_k_weight(jax.random.fold_in(streams_of[9], 71), part),
        "v_weight": gaussian(streams_of[3], (BLOCKS, HEADS, HEAD, HEAD), HEAD ** -0.5, 0.5, ((1, 2),)),
        "mod_base": gaussian(streams_of[4], (BLOCKS, 3, D), 0.5, 3.0, ((2, 2),), jnp.float32),
        "mod_amp": gaussian(streams_of[5], (BLOCKS, 3, D), 0.5, 3.0, ((2, 2),), jnp.float32),
        "levels": with_ends(jax.random.randint(part_keys[6], (QUEUE,), 0, STEPS), jax.random.fold_in(part_keys[6], 1), 0, STEPS - 1).astype(jnp.int32),
        "steps_table": with_ends(jax.random.randint(streams_of[7], (STEPS + 1,), 0, 1001), jax.random.fold_in(streams_of[7], 1), 0, 1000).astype(jnp.int32),
        "group_pos": with_ends(jax.random.randint(part_keys[8], (QUEUE,), 0, 4 * QUEUE), jax.random.fold_in(part_keys[8], 1), 0, (4 * QUEUE) - 1).astype(jnp.int32),
    }


def time_embed(moment, channel):
    within = channel % 256
    freq = jnp.exp(-jnp.log(10000.0) * (within % 128).astype(jnp.float32) / 128.0)
    angle = moment * freq
    return jnp.where(within < 128, jnp.cos(angle), jnp.sin(angle))

def angle_table(start, count):
    place = jnp.arange(count, dtype=jnp.int32)
    tpos = (start + place // HW_DEV).astype(jnp.float32)
    inner = place % HW_DEV
    hpos = (inner // WIDE).astype(jnp.float32)
    wpos = (inner % WIDE).astype(jnp.float32)
    side_pairs = HEAD // 6
    time_pairs = (HEAD - 4 * side_pairs) // 2
    freq_t = 10000.0 ** (-jnp.arange(time_pairs, dtype=jnp.float32) / time_pairs)
    freq_s = 10000.0 ** (-jnp.arange(side_pairs, dtype=jnp.float32) / side_pairs)
    return jnp.concatenate([tpos[:, None] * freq_t, hpos[:, None] * freq_s, wpos[:, None] * freq_s], axis=1)

def rotate(values, angles):
    count, heads, size = values.shape
    paired = values.reshape(count, heads, size // 2, 2)
    cosine = jnp.cos(angles)[:, None, :]
    sine = jnp.sin(angles)[:, None, :]
    first = paired[..., 0]
    second = paired[..., 1]
    turned = jnp.stack([first * cosine - second * sine, first * sine + second * cosine], axis=-1)
    return turned.reshape(count, heads, size)

def rms_rotate(raw, angles):
    total = lax.optimization_barrier(jnp.sum(raw * raw, axis=(1, 2)))
    scaled = raw * lax.rsqrt(total / D + 1e-06)[:, None, None]
    return rotate(scaled, angles).astype(jnp.bfloat16)

def attend_blocks(query, keys, values, valid, scale):
    count, heads, size = query.shape
    span = math.gcd(heads, 4)
    number = heads // span

    def one(block_index):
        qpart = lax.dynamic_slice_in_dim(query, block_index * span, span, 1).astype(jnp.float32)
        kpart = lax.dynamic_slice_in_dim(keys, block_index * span, span, 1).astype(jnp.float32)
        vpart = lax.dynamic_slice_in_dim(values, block_index * span, span, 1).astype(jnp.float32)
        scores = jnp.einsum('qhd,khd->hqk', qpart, kpart) * scale
        scores = jnp.where(valid[None, None, :], scores, jnp.float32(-1e+30))
        top = lax.optimization_barrier(jnp.max(scores, axis=-1, keepdims=True))
        expo = jnp.exp(scores - top)
        weights = (expo / lax.optimization_barrier(jnp.sum(expo, axis=-1, keepdims=True))).astype(jnp.bfloat16)
        return jnp.einsum('hqk,khd->qhd', weights.astype(jnp.float32), vpart)
    parts = lax.map(one, jnp.arange(number, dtype=jnp.int32))
    return jnp.transpose(parts, (1, 0, 2, 3)).reshape(count, heads * size)

def reference(hidden, q_weight, k_weight, v_weight, mod_base, mod_amp, levels, steps_table, group_pos):
    groups = hidden.reshape(QUEUE, TOK_DEV, D)
    state = groups.astype(jnp.float32)
    t_now = steps_table[levels].astype(jnp.float32)
    t_next = steps_table[levels + 1].astype(jnp.float32)
    channel = jnp.arange(D, dtype=jnp.int32)
    emb = time_embed(t_now[:, None], channel[None, :])
    scale = 1.0 / jnp.sqrt(jnp.float32(HEAD))
    for block in range(BLOCKS):
        mods = mod_base[block][None] + mod_amp[block][None] * emb[:, None, :]
        mean = lax.optimization_barrier(jnp.sum(state, axis=-1, keepdims=True)) / D
        second = lax.optimization_barrier(jnp.sum(state * state, axis=-1, keepdims=True)) / D
        normed = (state - mean) * lax.rsqrt(second - mean * mean + 1e-06)
        mixed = (normed * (1.0 + mods[:, 1:2, :]) + mods[:, 0:1, :]).astype(jnp.bfloat16)
        q_now = q_weight[block].astype(jnp.float32)
        k_now = k_weight[block].astype(jnp.float32)
        v_now = v_weight[block].astype(jnp.float32)

        def project(index):
            heads_here = mixed[index].reshape(TOK_DEV, HEADS, HEAD).astype(jnp.float32)
            angles = angle_table(group_pos[index], TOK_DEV)
            key_raw = jnp.einsum('thd,hde->the', heads_here, k_now)
            value = jnp.einsum('thd,hde->the', heads_here, v_now).astype(jnp.bfloat16)
            return (rms_rotate(key_raw, angles), value)
        all_keys, all_values = lax.map(project, jnp.arange(QUEUE, dtype=jnp.int32))

        def attend(index):
            before_index = jnp.maximum(index - 1, 0)
            after_index = jnp.minimum(index + 1, QUEUE - 1)
            own_heads = mixed[index].reshape(TOK_DEV, HEADS, HEAD).astype(jnp.float32)
            query_raw = jnp.einsum('thd,hde->the', own_heads, q_now)
            query = rms_rotate(query_raw, angle_table(group_pos[index], TOK_DEV))
            keys = jnp.concatenate([all_keys[before_index], all_keys[index], all_keys[after_index]], axis=0)
            values = jnp.concatenate([all_values[before_index], all_values[index], all_values[after_index]], axis=0)
            valid = jnp.concatenate([jnp.full((TOK_DEV,), index > 0), jnp.full((TOK_DEV,), True), jnp.full((TOK_DEV,), index < QUEUE - 1)])
            return attend_blocks(query, keys, values, valid, scale)
        attention = lax.map(attend, jnp.arange(QUEUE, dtype=jnp.int32))
        state = state + mods[:, 2:3, :] * attention
    velocity = state.astype(jnp.bfloat16)
    step_size = (t_next - t_now) / 1000.0
    advanced = (groups.astype(jnp.float32) + step_size[:, None, None] * state).astype(jnp.bfloat16)
    new_queue = jnp.concatenate([jnp.zeros((1, TOK_DEV, D), jnp.bfloat16), advanced[:-1]], axis=0)
    return (new_queue.reshape(TOKENS, D), velocity.reshape(TOKENS, D))
```

```python
import functools
import math

import jax
import jax.numpy as jnp
from jax import lax
from jax.experimental import pallas as pl
from jax.experimental.pallas import tpu as pltpu
from jax.sharding import PartitionSpec as P

HEAD = 128
D = 5120
WIDE = 52
HW_DEV = 104
F32 = jnp.float32
BF16 = jnp.bfloat16


def time_embed(moment, channel):
    within = channel % 256
    freq = jnp.exp(-jnp.log(10000.0) * (within % 128).astype(F32) / 128.0)
    angle = moment * freq
    return jnp.where(within < 128, jnp.cos(angle), jnp.sin(angle))


def turn_tables(starts, count):
    place = jnp.arange(count, dtype=jnp.int32)
    inner = place % HW_DEV
    frame = (place // HW_DEV)[:, None]
    hpos = (inner // WIDE).astype(F32)[:, None]
    wpos = (inner % WIDE).astype(F32)[:, None]
    lane = jnp.arange(HEAD, dtype=jnp.int32)
    pair = lane // 2
    side = HEAD // 6
    time = (HEAD - 4 * side) // 2
    freq_t = 10000.0 ** (-pair.astype(F32) / time)
    freq_h = 10000.0 ** (-(pair - time).astype(F32) / side)
    freq_w = 10000.0 ** (-(pair - time - side).astype(F32) / side)
    tpos = (starts[:, None, None] + frame[None]).astype(F32)
    on_t = (pair < time)[None, None, :]
    on_h = (pair < time + side)[None, None, :]
    angle = jnp.where(
        on_t,
        tpos * freq_t[None, None, :],
        jnp.where(on_h, (hpos * freq_h[None, :])[None], (wpos * freq_w[None, :])[None]),
    )
    sign = jnp.where(lane % 2 == 0, -1.0, 1.0).astype(F32)
    return jnp.cos(angle), jnp.sin(angle) * sign[None, None, :]


def kernel(
    chunks, length,
    hid, wq, wk, wv, mods, sendmods, cost, sint,
    newq, vel,
    near, far, nmods, fmods, tsend, trecv, nstat, fstat, ostat,
    qrot, krot, vown, wk2, qsq, ksq, adv, kcat, vcat,
    hs, hr, fs, fr, tss, trs, mss, mrs, sss, srs, avs, avr,
):
    rows, width = hid.shape
    heads = width // HEAD
    per = heads // chunks
    cw = per * HEAD
    me = lax.axis_index("queue")
    core = lax.axis_index("tp")
    odd = lax.rem(me, 2)
    s = 1 - 2 * odd
    has_far = jnp.logical_and(me - s >= 0, me - s < length)
    has_fwd = jnp.logical_and(me + 2 * s >= 0, me + 2 * s < length)
    has_src = has_far

    def clip(j):
        return jnp.minimum(jnp.maximum(j, 0), length - 1)

    dev_near = {"queue": clip(me + s)}
    dev_far = {"queue": clip(me - s)}
    dev_fwd = {"queue": clip(me + 2 * s)}
    dev_src = {"queue": clip(me - 2 * s)}
    dev_next = {"queue": clip(me + 1)}
    partner = {"tp": 1 - core}
    MESH = pl.DeviceIdType.MESH

    barrier = pltpu.get_barrier_semaphore()
    pl.semaphore_signal(barrier, inc=1, device_id=partner, device_id_type=MESH)
    pl.semaphore_signal(barrier, inc=1, device_id=dev_near, device_id_type=MESH)

    @pl.when(has_far)
    def _():
        pl.semaphore_signal(barrier, inc=1, device_id=dev_far, device_id_type=MESH)
        pl.semaphore_signal(barrier, inc=1, device_id=dev_src, device_id_type=MESH)

    @pl.when(has_fwd)
    def _():
        pl.semaphore_signal(barrier, inc=1, device_id=dev_fwd, device_id_type=MESH)

    peers = 2 + jnp.where(has_far, 2, 0) + jnp.where(has_fwd, 1, 0)
    pl.semaphore_wait(barrier, peers)

    def cols(c):
        return pl.ds(pl.multiple_of(c * cw, cw), cw)

    def hcols(h):
        return pl.ds(pl.multiple_of(h * HEAD, HEAD), HEAD)

    def remote(src, dst, ss, rs, dev):
        return pltpu.make_async_remote_copy(
            src_ref=src, dst_ref=dst, send_sem=ss, recv_sem=rs, device_id=dev, device_id_type=MESH
        )

    def hid_copy(c):
        return remote(hid.at[:, cols(c)], near.at[:, cols(c)], hs.at[c], hr.at[c], dev_near)

    def fwd_copy(c):
        return remote(near.at[:, cols(c)], far.at[:, cols(c)], fs.at[c], fr.at[c], dev_fwd)

    def adv_copy(c):
        return remote(adv.at[:, cols(c)], newq.at[:, cols(c)], avs.at[c], avr.at[c], dev_next)

    mod_near = remote(sendmods, nmods, mss.at[0], mrs.at[0], dev_near)
    mod_far = remote(sendmods, fmods, mss.at[1], mrs.at[1], dev_far)
    stat_near = remote(ostat, nstat, sss.at[0], srs.at[0], dev_near)
    stat_far = remote(ostat, fstat, sss.at[1], srs.at[1], dev_far)
    tot0 = remote(tsend.at[0:2], trecv.at[0:2], tss.at[0], trs.at[0], partner)
    tot1 = remote(tsend.at[2:4], trecv.at[2:4], tss.at[1], trs.at[1], partner)

    mod_near.start()

    @pl.when(has_far)
    def _():
        mod_far.start()

    @pl.loop(0, chunks)
    def _(c):
        hid_copy(c).start()

    def forward(c):
        hid_copy(c).wait_recv()

        @pl.when(has_fwd)
        def _():
            fwd_copy(c).start()

    tsend[0] = jnp.zeros((rows, HEAD), F32)
    tsend[1] = jnp.zeros((rows, HEAD), F32)

    @pl.loop(0, heads)
    def _(h):
        x = hid[:, hcols(h)].astype(F32)
        tsend[0] += x
        tsend[1] += x * x

    tot0.start()

    lane = lax.broadcasted_iota(jnp.int32, (rows, HEAD), 1)
    swap = (
        lax.broadcasted_iota(jnp.int32, (HEAD, HEAD), 0)
        == (lax.broadcasted_iota(jnp.int32, (HEAD, HEAD), 1) ^ 1)
    ).astype(F32).astype(BF16)
    keys = kcat.shape[0]
    kcat[3 * rows:, :] = jnp.zeros((keys - 3 * rows, HEAD), BF16)
    vcat[:, HEAD:] = jnp.ones((keys, HEAD), BF16)
    vcat[3 * rows:, :HEAD] = jnp.zeros((keys - 3 * rows, HEAD), BF16)
    key_lane = lax.broadcasted_iota(jnp.int32, (1, keys), 1)
    limit = jnp.where(has_far, 3 * rows, 2 * rows)
    bias = jnp.where(key_lane < limit, 0.0, -1e30).astype(F32)

    @pl.when(jnp.logical_not(has_far))
    def _():
        far[...] = jnp.zeros_like(far)
        fmods[...] = jnp.zeros_like(fmods)
        fstat[...] = jnp.zeros_like(fstat)

    @pl.when(me == 0)
    def _():
        newq[...] = jnp.zeros_like(newq)

    qsq[...] = jnp.zeros_like(qsq)
    ksq[...] = jnp.zeros_like(ksq)
    tot0.wait()
    total = jnp.sum(tsend[0] + trecv[0], axis=1, keepdims=True)
    second = jnp.sum(tsend[1] + trecv[1], axis=1, keepdims=True)
    mean = total / D
    rstd = lax.rsqrt(second / D - mean * mean + 1e-06)
    ostat[...] = jnp.where(lane == 0, mean, rstd)

    def mix(x, mu, rs, scale, shift):
        return ((x.astype(F32) - mu) * rs * (1.0 + scale) + shift).astype(BF16)

    def dot(a, b):
        return jnp.dot(a, b, preferred_element_type=F32)

    def own(h):
        mu = ostat[:, 0:1]
        rs = ostat[:, 1:2]
        mixed = mix(hid[:, hcols(h)], mu, rs, mods[1:2, hcols(h)], mods[0:1, hcols(h)])
        q = wq[h]
        k = wk[h]
        q2 = jnp.concatenate([q, dot(q, swap).astype(BF16)], axis=1)
        k2 = jnp.concatenate([k, dot(k, swap).astype(BF16)], axis=1)
        wk2[h] = k2
        qraw = dot(mixed, q2)
        kraw = dot(mixed, k2)
        q1 = qraw[:, :HEAD]
        k1 = kraw[:, :HEAD]
        qsq[...] += q1 * q1
        ksq[...] += k1 * k1
        qrot[h] = q1 * cost[0] + qraw[:, HEAD:] * sint[0]
        krot[h] = k1 * cost[0] + kraw[:, HEAD:] * sint[0]
        vown[h] = dot(mixed, wv[h]).astype(BF16)

    half = heads // 2

    @pl.loop(0, half)
    def _(h):
        own(h)

    ahead = min(3, chunks)
    forward(0)

    @pl.loop(half, heads)
    def _(h):
        own(h)

    tsend[2] = qsq[...]
    tsend[3] = ksq[...]
    tot1.start()

    @pl.loop(1, ahead)
    def _(c):
        forward(c)

    tot1.wait()
    qt = jnp.sum(tsend[2] + trecv[2], axis=1, keepdims=True)
    kt = jnp.sum(tsend[3] + trecv[3], axis=1, keepdims=True)
    rq = lax.rsqrt(qt / D + 1e-06)
    rk = lax.rsqrt(kt / D + 1e-06)
    qsq[...] = jnp.broadcast_to(rq, (rows, HEAD))
    ksq[...] = jnp.broadcast_to(rk, (rows, HEAD))
    ostat[...] = jnp.where(lane == 2, rk, ostat[...])
    stat_near.start()

    @pl.when(has_far)
    def _():
        stat_far.start()

    mod_near.wait()
    stat_near.wait()

    @pl.when(has_far)
    def _():
        mod_far.wait()
        stat_far.wait()

    factor = math.log2(math.e) / math.sqrt(HEAD)

    def other(h, slot, buf, stat, md):
        mixed = mix(buf[:, hcols(h)], stat[:, 0:1], stat[:, 1:2], md[1:2, hcols(h)], md[0:1, hcols(h)])
        kraw = dot(mixed, wk2[h])
        rk = stat[:, 2:3]
        turned = kraw[:, :HEAD] * cost[slot] + kraw[:, HEAD:] * sint[slot]
        kcat[slot * rows:(slot + 1) * rows, :] = (turned * rk).astype(BF16)
        vcat[slot * rows:(slot + 1) * rows, :HEAD] = dot(mixed, wv[h]).astype(BF16)

    def head(h):
        query = (qrot[h] * qsq[...]).astype(BF16)
        kcat[0:rows, :] = (krot[h] * ksq[...]).astype(BF16)
        vcat[0:rows, :HEAD] = vown[h]
        other(h, 1, near, nstat, nmods)
        other(h, 2, far, fstat, fmods)
        scores = lax.dot_general(
            query, kcat[...], (((1,), (1,)), ((), ())), preferred_element_type=F32
        )
        scores = scores * factor + bias
        top = jnp.max(scores, axis=1, keepdims=True)
        weights = jnp.exp2(scores - top).astype(BF16)
        out = dot(weights, vcat[...])
        attn = out[:, :HEAD] / out[:, HEAD:]
        x = hid[:, hcols(h)].astype(F32)
        state = x + mods[2:3, hcols(h)] * attn
        vel[:, hcols(h)] = state.astype(BF16)
        adv[:, hcols(h)] = (x + mods[3:4, hcols(h)] * state).astype(BF16)

    has_next = me < length - 1

    @pl.loop(0, chunks)
    def _(c):
        @pl.when(c + ahead < chunks)
        def _():
            forward(c + ahead)

        @pl.when(has_far)
        def _():
            fwd_copy(c).wait_recv()

        @pl.loop(0, per)
        def _(n):
            head(c * per + n)

        @pl.when(jnp.logical_and(has_next, c > 0))
        def _():
            adv_copy(c - 1).start()

    @pl.when(has_next)
    def _():
        adv_copy(chunks - 1).start()

    @pl.loop(0, chunks)
    def _(c):
        hid_copy(c).wait_send()

        @pl.when(has_fwd)
        def _():
            fwd_copy(c).wait_send()

        @pl.when(has_next)
        def _():
            adv_copy(c).wait_send()

        @pl.when(me > 0)
        def _():
            adv_copy(c).wait_recv()


def body(length, hidden, q_weight, k_weight, v_weight, mod_base, mod_amp, levels, steps_table, group_pos):
    rows, width = hidden.shape
    heads = width // HEAD
    chunks = next(n for n in (10, 5, 4, 2, 1) if heads % n == 0)
    position = lax.axis_index("queue")
    t_now = steps_table[levels[0]].astype(F32)
    t_next = steps_table[levels[0] + 1].astype(F32)
    channel = lax.axis_index("tp") * width + jnp.arange(width, dtype=jnp.int32)
    emb = time_embed(t_now, channel)
    mods = mod_base[0] + mod_amp[0] * emb[None, :]
    step = jnp.full((1, width), (t_next - t_now) / 1000.0, F32)
    sendmods = mods[:2]
    mods = jnp.concatenate([mods, step], axis=0)
    s = 1 - 2 * (position % 2)
    slots = jnp.stack([position, position + s, position - s])
    starts = group_pos[jnp.clip(slots, 0, length - 1)]
    cost, sint = turn_tables(starts, rows)
    keys = -(-3 * rows // 128) * 128
    vmem = pl.BlockSpec(memory_space=pltpu.VMEM)
    dma = pltpu.SemaphoreType.DMA
    return pl.pallas_call(
        functools.partial(kernel, chunks, length),
        name="denoise",
        out_shape=(
            jax.ShapeDtypeStruct((rows, width), BF16),
            jax.ShapeDtypeStruct((rows, width), BF16),
        ),
        in_specs=[vmem] * 8,
        out_specs=(vmem, vmem),
        scratch_shapes=[
            pltpu.VMEM((rows, width), BF16),
            pltpu.VMEM((rows, width), BF16),
            pltpu.VMEM((2, width), F32),
            pltpu.VMEM((2, width), F32),
            pltpu.VMEM((4, rows, HEAD), F32),
            pltpu.VMEM((4, rows, HEAD), F32),
            pltpu.VMEM((rows, HEAD), F32),
            pltpu.VMEM((rows, HEAD), F32),
            pltpu.VMEM((rows, HEAD), F32),
            pltpu.VMEM((heads, rows, HEAD), F32),
            pltpu.VMEM((heads, rows, HEAD), F32),
            pltpu.VMEM((heads, rows, HEAD), BF16),
            pltpu.VMEM((heads, HEAD, 2 * HEAD), BF16),
            pltpu.VMEM((rows, HEAD), F32),
            pltpu.VMEM((rows, HEAD), F32),
            pltpu.VMEM((rows, width), BF16),
            pltpu.VMEM((keys, HEAD), BF16),
            pltpu.VMEM((keys, 2 * HEAD), BF16),
            dma((chunks,)), dma((chunks,)), dma((chunks,)), dma((chunks,)),
            dma((2,)), dma((2,)), dma((2,)), dma((2,)), dma((2,)), dma((2,)),
            dma((chunks,)), dma((chunks,)),
        ],
        compiler_params=pltpu.CompilerParams(
            collective_id=0, has_side_effects=True, vmem_limit_bytes=48 * 1024 * 1024
        ),
    )(hidden, q_weight[0], k_weight[0], v_weight[0], mods, sendmods, cost, sint)


def solution(mesh):
    length = mesh.shape["queue"]
    return jax.shard_map(
        functools.partial(body, length),
        mesh=mesh,
        in_specs=(
            P(("groups", "queue"), "tp"),
            P(None, "tp", None, None),
            P(None, "tp", None, None),
            P(None, "tp", None, None),
            P(None, None, "tp"),
            P(None, None, "tp"),
            P(("groups", "queue")),
            P(),
            P("groups"),
        ),
        out_specs=(P(("groups", "queue"), "tp"), P(("groups", "queue"), "tp")),
        check_vma=False,
    )
```

```python
import functools
import math

import jax
import jax.numpy as jnp
from jax import lax
from jax.experimental import pallas as pl
from jax.experimental.pallas import tpu as pltpu
from jax.sharding import PartitionSpec as P

HEAD = 128
D = 5120
WIDE = 52
HW_DEV = 104
F32 = jnp.float32
BF16 = jnp.bfloat16


def turn_freq():
    pair = jnp.arange(HEAD, dtype=jnp.int32) // 2
    side = HEAD // 6
    time = (HEAD - 4 * side) // 2
    freq_t = 10000.0 ** (-pair.astype(F32) / time)
    freq_h = 10000.0 ** (-(pair - time).astype(F32) / side)
    freq_w = 10000.0 ** (-(pair - time - side).astype(F32) / side)
    return jnp.where(pair < time, freq_t, jnp.where(pair < time + side, freq_h, freq_w))[None]


def kernel(
    chunks, length,
    hid_in, wq_in, wk_in, wv_in, base, amp, cfreq, tfreq, levels, steps, gpos,
    newq, vel,
    near, far, nmods, fmods, tsend, trecv, nstat, fstat, ostat,
    qrot, krot, vown, wk2, qsq, ksq, adv, kcat, vcat,
    hid, wq, wk, wv, mods, sendmods, cost, sint, mstat, wide, ins,
    hs, hr, fs, fr, tss, trs, mss, mrs, sss, srs, avs, avr,
):
    rows, width = hid_in.shape
    heads = width // HEAD
    per = heads // chunks
    cw = per * HEAD
    loads = [
        pltpu.make_async_copy(src, dst, ins.at[n])
        for n, (src, dst) in enumerate(((hid_in, hid), (wq_in, wq), (wk_in, wk), (wv_in, wv)))
    ]
    for load in loads:
        load.start()
    me = lax.axis_index("queue")
    core = lax.axis_index("tp")
    odd = lax.rem(me, 2)
    s = 1 - 2 * odd
    has_far = jnp.logical_and(me - s >= 0, me - s < length)
    has_fwd = jnp.logical_and(me + 2 * s >= 0, me + 2 * s < length)
    has_src = has_far

    def clip(j):
        return jnp.minimum(jnp.maximum(j, 0), length - 1)

    dev_near = {"queue": clip(me + s)}
    dev_far = {"queue": clip(me - s)}
    dev_fwd = {"queue": clip(me + 2 * s)}
    dev_src = {"queue": clip(me - 2 * s)}
    dev_next = {"queue": clip(me + 1)}
    partner = {"tp": 1 - core}
    MESH = pl.DeviceIdType.MESH

    barrier = pltpu.get_barrier_semaphore()
    pl.semaphore_signal(barrier, inc=1, device_id=partner, device_id_type=MESH)
    pl.semaphore_signal(barrier, inc=1, device_id=dev_near, device_id_type=MESH)

    @pl.when(has_far)
    def _():
        pl.semaphore_signal(barrier, inc=1, device_id=dev_far, device_id_type=MESH)
        pl.semaphore_signal(barrier, inc=1, device_id=dev_src, device_id_type=MESH)

    @pl.when(has_fwd)
    def _():
        pl.semaphore_signal(barrier, inc=1, device_id=dev_fwd, device_id_type=MESH)

    peers = 2 + jnp.where(has_far, 2, 0) + jnp.where(has_fwd, 1, 0)
    pl.semaphore_wait(barrier, peers)

    def cols(c):
        return pl.ds(pl.multiple_of(c * cw, cw), cw)

    def hcols(h):
        return pl.ds(pl.multiple_of(h * HEAD, HEAD), HEAD)

    def remote(src, dst, ss, rs, dev):
        return pltpu.make_async_remote_copy(
            src_ref=src, dst_ref=dst, send_sem=ss, recv_sem=rs, device_id=dev, device_id_type=MESH
        )

    def hid_copy(c):
        return remote(hid.at[:, cols(c)], near.at[:, cols(c)], hs.at[c], hr.at[c], dev_near)

    def fwd_copy(c):
        return remote(near.at[:, cols(c)], far.at[:, cols(c)], fs.at[c], fr.at[c], dev_fwd)

    def adv_copy(c):
        return remote(adv.at[:, cols(c)], newq.at[:, cols(c)], avs.at[c], avr.at[c], dev_next)

    mod_near = remote(sendmods, nmods, mss.at[0], mrs.at[0], dev_near)
    mod_far = remote(sendmods, fmods, mss.at[1], mrs.at[1], dev_far)
    stat_near = remote(mstat, nstat, sss.at[0], srs.at[0], dev_near)
    stat_far = remote(mstat, fstat, sss.at[1], srs.at[1], dev_far)
    tot0 = remote(tsend.at[0:2], trecv.at[0:2], tss.at[0], trs.at[0], partner)
    tot1 = remote(tsend.at[2:4], trecv.at[2:4], tss.at[1], trs.at[1], partner)

    loads[0].wait()

    @pl.loop(0, chunks)
    def _(c):
        hid_copy(c).start()

    now = steps[levels[0]].astype(F32)
    ahead_t = steps[levels[0] + 1].astype(F32)
    channel = lax.broadcasted_iota(jnp.int32, (1, width), 1) + core * width
    phase = cfreq[...] * now
    emb = jnp.where((channel & 255) < 128, jnp.cos(phase), jnp.sin(phase))
    own_mods = base[...] + amp[...] * emb
    sendmods[...] = own_mods[0:2]
    mods[0:3] = own_mods
    mods[3:4] = jnp.broadcast_to((ahead_t - now) / 1000.0, (1, width))

    def forward(c):
        hid_copy(c).wait_recv()

        @pl.when(has_fwd)
        def _():
            fwd_copy(c).start()

    tsend[0] = jnp.zeros((rows, HEAD), F32)
    tsend[1] = jnp.zeros((rows, HEAD), F32)

    @pl.loop(0, heads)
    def _(h):
        x = hid[:, hcols(h)].astype(F32)
        tsend[0] += x
        tsend[1] += x * x

    tot0.start()
    mod_near.start()

    @pl.when(has_far)
    def _():
        mod_far.start()

    place = lax.broadcasted_iota(jnp.int32, (rows, HEAD), 0)
    frame = jnp.zeros_like(place)
    for n in range(1, rows // HW_DEV):
        frame += (place >= n * HW_DEV).astype(jnp.int32)
    inner = place - frame * HW_DEV
    hpos = jnp.zeros_like(place)
    for n in range(1, HW_DEV // WIDE):
        hpos += (inner >= n * WIDE).astype(jnp.int32)
    wpos = inner - hpos * WIDE
    spot = lax.broadcasted_iota(jnp.int32, (rows, HEAD), 1)
    pair = lax.shift_right_logical(spot, 1)
    side = HEAD // 6
    time = (HEAD - 4 * side) // 2
    rest = jnp.where(pair < time + side, hpos, wpos)
    sign = jnp.where((spot & 1) == 0, -1.0, 1.0).astype(F32)
    for slot, owner in enumerate((me, me + s, me - s)):
        moment = jnp.where(pair < time, gpos[clip(owner)] + frame, rest).astype(F32)
        angle = moment * tfreq[...]
        cost[slot] = jnp.cos(angle)
        sint[slot] = jnp.sin(angle) * sign

    lane = lax.broadcasted_iota(jnp.int32, (rows, HEAD), 1)
    swap = (
        lax.broadcasted_iota(jnp.int32, (HEAD, HEAD), 0)
        == (lax.broadcasted_iota(jnp.int32, (HEAD, HEAD), 1) ^ 1)
    ).astype(F32).astype(BF16)
    keys = kcat.shape[0]
    kcat[3 * rows:, :] = jnp.zeros((keys - 3 * rows, HEAD), BF16)
    vcat[:, HEAD:] = jnp.ones((keys, HEAD), BF16)
    vcat[3 * rows:, :HEAD] = jnp.zeros((keys - 3 * rows, HEAD), BF16)
    key_lane = lax.broadcasted_iota(jnp.int32, (1, keys), 1)
    limit = jnp.where(has_far, 3 * rows, 2 * rows)
    bias = jnp.where(key_lane < limit, 0.0, -1e30).astype(F32)

    @pl.when(jnp.logical_not(has_far))
    def _():
        far[...] = jnp.zeros_like(far)
        fmods[...] = jnp.zeros_like(fmods)
        fstat[...] = jnp.zeros_like(fstat)

    @pl.when(me == 0)
    def _():
        newq[...] = jnp.zeros_like(newq)

    qsq[...] = jnp.zeros_like(qsq)
    ksq[...] = jnp.zeros_like(ksq)
    tot0.wait()
    total = jnp.sum(tsend[0] + trecv[0], axis=1, keepdims=True)
    second = jnp.sum(tsend[1] + trecv[1], axis=1, keepdims=True)
    mean = total / D
    rstd = lax.rsqrt(second / D - mean * mean + 1e-06)
    ostat[...] = jnp.where(lane == 0, mean, rstd)

    def mix(x, mu, rs, scale, shift):
        return ((x.astype(F32) - mu) * rs * (1.0 + scale) + shift).astype(BF16)

    def dot(a, b):
        return jnp.dot(a, b, preferred_element_type=F32)

    def own(h):
        mu = ostat[:, 0:1]
        rs = ostat[:, 1:2]
        mixed = mix(hid[:, hcols(h)], mu, rs, mods[1:2, hcols(h)], mods[0:1, hcols(h)])
        q = wq[h]
        k = wk[h]
        q2 = jnp.concatenate([q, dot(q, swap).astype(BF16)], axis=1)
        k2 = jnp.concatenate([k, dot(k, swap).astype(BF16)], axis=1)
        wk2[h] = k2
        qraw = dot(mixed, q2)
        kraw = dot(mixed, k2)
        q1 = qraw[:, :HEAD]
        k1 = kraw[:, :HEAD]
        qsq[...] += q1 * q1
        ksq[...] += k1 * k1
        qrot[h] = q1 * cost[0] + qraw[:, HEAD:] * sint[0]
        krot[h] = k1 * cost[0] + kraw[:, HEAD:] * sint[0]
        vown[h] = dot(mixed, wv[h]).astype(BF16)

    for load in loads[1:]:
        load.wait()

    half = heads // 2

    @pl.loop(0, half)
    def _(h):
        own(h)

    ahead = min(3, chunks)
    forward(0)

    @pl.loop(half, heads)
    def _(h):
        own(h)

    tsend[2] = qsq[...]
    tsend[3] = ksq[...]
    tot1.start()

    @pl.loop(1, ahead)
    def _(c):
        forward(c)

    tot1.wait()
    qt = jnp.sum(tsend[2] + trecv[2], axis=1, keepdims=True)
    kt = jnp.sum(tsend[3] + trecv[3], axis=1, keepdims=True)
    rq = lax.rsqrt(qt / D + 1e-06)
    rk = lax.rsqrt(kt / D + 1e-06)
    qsq[...] = jnp.broadcast_to(rq, (rows, HEAD))
    ksq[...] = jnp.broadcast_to(rk, (rows, HEAD))
    ostat[...] = jnp.where(lane == 2, rk, ostat[...])
    wide[...] = jnp.zeros_like(wide)
    wide[0:rows] = ostat[...]
    mstat[...] = jnp.transpose(wide[...])[0:8]
    stat_near.start()

    @pl.when(has_far)
    def _():
        stat_far.start()

    mod_near.wait()
    stat_near.wait()

    @pl.when(has_far)
    def _():
        mod_far.wait()
        stat_far.wait()

    def spread(stat, place_at):
        full = jnp.concatenate([stat[...], jnp.zeros((HEAD - 8, stat.shape[1]), F32)], axis=0)
        place_at[...] = jnp.transpose(full)[0:rows]

    spread(nstat, trecv.at[0])
    spread(fstat, trecv.at[1])
    near_stat = trecv.at[0]
    far_stat = trecv.at[1]

    factor = math.log2(math.e) / math.sqrt(HEAD)

    def other(h, slot, buf, stat, md):
        mixed = mix(buf[:, hcols(h)], stat[:, 0:1], stat[:, 1:2], md[1:2, hcols(h)], md[0:1, hcols(h)])
        kraw = dot(mixed, wk2[h])
        rk = stat[:, 2:3]
        turned = kraw[:, :HEAD] * cost[slot] + kraw[:, HEAD:] * sint[slot]
        kcat[slot * rows:(slot + 1) * rows, :] = (turned * rk).astype(BF16)
        vcat[slot * rows:(slot + 1) * rows, :HEAD] = dot(mixed, wv[h]).astype(BF16)

    def head(h):
        query = (qrot[h] * qsq[...]).astype(BF16)
        kcat[0:rows, :] = (krot[h] * ksq[...]).astype(BF16)
        vcat[0:rows, :HEAD] = vown[h]
        other(h, 1, near, near_stat, nmods)
        other(h, 2, far, far_stat, fmods)
        scores = lax.dot_general(
            query, kcat[...], (((1,), (1,)), ((), ())), preferred_element_type=F32
        )
        scores = scores * factor + bias
        top = jnp.max(scores, axis=1, keepdims=True)
        weights = jnp.exp2(scores - top).astype(BF16)
        out = dot(weights, vcat[...])
        attn = out[:, :HEAD] / out[:, HEAD:]
        x = hid[:, hcols(h)].astype(F32)
        state = x + mods[2:3, hcols(h)] * attn
        vel[:, hcols(h)] = state.astype(BF16)
        adv[:, hcols(h)] = (x + mods[3:4, hcols(h)] * state).astype(BF16)

    has_next = me < length - 1

    @pl.loop(0, chunks)
    def _(c):
        @pl.when(c + ahead < chunks)
        def _():
            forward(c + ahead)

        @pl.when(has_far)
        def _():
            fwd_copy(c).wait_recv()

        @pl.loop(0, per)
        def _(n):
            head(c * per + n)

        @pl.when(jnp.logical_and(has_next, c > 0))
        def _():
            adv_copy(c - 1).start()

    @pl.when(has_next)
    def _():
        adv_copy(chunks - 1).start()

    @pl.loop(0, chunks)
    def _(c):
        hid_copy(c).wait_send()

        @pl.when(has_fwd)
        def _():
            fwd_copy(c).wait_send()

        @pl.when(has_next)
        def _():
            adv_copy(c).wait_send()

        @pl.when(me > 0)
        def _():
            adv_copy(c).wait_recv()


def body(length, hidden, q_weight, k_weight, v_weight, mod_base, mod_amp, levels, steps_table, group_pos):
    rows, width = hidden.shape
    heads = width // HEAD
    chunks = next(n for n in (10, 5, 4, 2, 1) if heads % n == 0)
    channel = lax.axis_index("tp") * width + jnp.arange(width, dtype=jnp.int32)
    within = channel % 256
    cfreq = jnp.exp(-jnp.log(10000.0) * (within % 128).astype(F32) / 128.0)[None]
    tall = -(-rows // 128) * 128
    keys = -(-3 * rows // 128) * 128
    vmem = pl.BlockSpec(memory_space=pltpu.VMEM)
    dma = pltpu.SemaphoreType.DMA
    return pl.pallas_call(
        functools.partial(kernel, chunks, length),
        name="denoise",
        out_shape=(
            jax.ShapeDtypeStruct((rows, width), BF16),
            jax.ShapeDtypeStruct((rows, width), BF16),
        ),
        in_specs=[pl.BlockSpec(memory_space=pl.ANY)] * 4
        + [vmem] * 4
        + [pl.BlockSpec(memory_space=pltpu.SMEM)] * 3,
        out_specs=(vmem, vmem),
        scratch_shapes=[
            pltpu.VMEM((rows, width), BF16),
            pltpu.VMEM((rows, width), BF16),
            pltpu.VMEM((2, width), F32),
            pltpu.VMEM((2, width), F32),
            pltpu.VMEM((4, rows, HEAD), F32),
            pltpu.VMEM((4, rows, HEAD), F32),
            pltpu.VMEM((8, tall), F32),
            pltpu.VMEM((8, tall), F32),
            pltpu.VMEM((rows, HEAD), F32),
            pltpu.VMEM((heads, rows, HEAD), F32),
            pltpu.VMEM((heads, rows, HEAD), F32),
            pltpu.VMEM((heads, rows, HEAD), BF16),
            pltpu.VMEM((heads, HEAD, 2 * HEAD), BF16),
            pltpu.VMEM((rows, HEAD), F32),
            pltpu.VMEM((rows, HEAD), F32),
            pltpu.VMEM((rows, width), BF16),
            pltpu.VMEM((keys, HEAD), BF16),
            pltpu.VMEM((keys, 2 * HEAD), BF16),
            pltpu.VMEM((rows, width), BF16),
            pltpu.VMEM((heads, HEAD, HEAD), BF16),
            pltpu.VMEM((heads, HEAD, HEAD), BF16),
            pltpu.VMEM((heads, HEAD, HEAD), BF16),
            pltpu.VMEM((4, width), F32),
            pltpu.VMEM((2, width), F32),
            pltpu.VMEM((3, rows, HEAD), F32),
            pltpu.VMEM((3, rows, HEAD), F32),
            pltpu.VMEM((8, tall), F32),
            pltpu.VMEM((tall, HEAD), F32),
            dma((4,)),
            dma((chunks,)), dma((chunks,)), dma((chunks,)), dma((chunks,)),
            dma((2,)), dma((2,)), dma((2,)), dma((2,)), dma((2,)), dma((2,)),
            dma((chunks,)), dma((chunks,)),
        ],
        compiler_params=pltpu.CompilerParams(
            collective_id=0, has_side_effects=True, vmem_limit_bytes=48 * 1024 * 1024
        ),
    )(
        hidden, q_weight[0], k_weight[0], v_weight[0], mod_base[0], mod_amp[0],
        cfreq, turn_freq(), levels, steps_table, group_pos,
    )


def solution(mesh):
    length = mesh.shape["queue"]
    return jax.shard_map(
        functools.partial(body, length),
        mesh=mesh,
        in_specs=(
            P(("groups", "queue"), "tp"),
            P(None, "tp", None, None),
            P(None, "tp", None, None),
            P(None, "tp", None, None),
            P(None, None, "tp"),
            P(None, None, "tp"),
            P(("groups", "queue")),
            P(),
            P("groups"),
        ),
        out_specs=(P(("groups", "queue"), "tp"), P(("groups", "queue"), "tp")),
        check_vma=False,
    )
```
